32 devices in a mesh: seq: 8 (over z, x), tp: 4 (over y, core).
Axes of the slice: x: 2, y: 2, z: 4, core: 2. Of those that a mesh axis runs over, the one named last changes fastest.
Arguments:
- tree_hidden: bfloat16 [16, 8192], P(None, 'seq'), may hold values from -6 to 6
- query_low: bfloat16 [16, 8192], P('seq', 'tp'), may hold values from -24 to 24
- key_tree_low: bfloat16 [16, 1024], P('seq', 'tp'), may hold values from -20 to 20
- value_tree_low: bfloat16 [16, 1024], P('seq', 'tp'), may hold values from -6 to 6
- cache_keys: bfloat16 [1, 8192, 8, 128], P(None, 'seq', 'tp'), may hold values from -40 to 40
- cache_values: bfloat16 [1, 8192, 8, 128], P(None, 'seq', 'tp'), may hold values from -6 to 6
- cache_lengths: int32 [1], replicated, may hold values from 1024 to 8192
- ancestors: int32 [1, 16, 16], replicated, may hold values from 0 to 1, as said below
- out_weight: bfloat16 [8192, 8192], P('tp', 'seq'), may hold values from -0.0625 to 0.0625
- norm_gain: float32 [8192], P('seq'), may hold values from 0.1 to 1.9
- w_query_up: bfloat16 [8192, 8192], P('seq', 'tp'), may hold values from -0.0625 to 0.0625
- w_key_up: bfloat16 [8192, 1024], P('seq', 'tp'), may hold values from -0.5 to 0.5
- w_value_up: bfloat16 [8192, 1024], P('seq', 'tp'), may hold values from -0.0625 to 0.0625
- retained_keys: bfloat16 [8, 512, 8, 128], P('seq', None, 'tp'), may hold values from -400 to 400
- retained_values: bfloat16 [8, 512, 8, 128], P('seq', None, 'tp'), may hold values from -6 to 6
- retained_index: int32 [8, 512, 8], P('seq', None, 'tp'), may hold values from 0 to 8191
Outputs:
- residual: float32 [16, 8192], P(None, 'seq')
- upper_heads: float32 [16, 8192], P('seq', 'tp')
The draws below stay inside these ranges and needn't reach their ends.
Inputs may be any that keep to these rules, and one draw needn't show every extreme that they name: ancestors[r, i, j] is 1 when node j is node i or an ancestor of node i in request r's tree, else 0; node 0 is the root and every other node's parent has a lower number.
All inputs are finite; a program needn't handle non-finite values.
Results may differ from the reference program's by a relative error of at most 0.04.
Values may be sent and summed in bfloat16 or wider, within the bound.
A program may use at most 64 MiB of HBM per device.

```python
import jax
import jax.numpy as jnp
from jax import lax

D = 8192
HQ = 64
KVH = 8
HD = 128
NODES = 16
GROUP = 8
RET = 4096
R = 1
M = 16
CACHE = 8192
RET_PART = 512


def tree_queries(key):
    drawn = jax.random.normal(jax.random.fold_in(key, 101), (R * NODES, HQ * HD), jnp.float32) * 4.0
    return jnp.clip(drawn, -24.0, 24.0)


def draw_query_low(key, part):
    return tree_queries(key).astype(jnp.bfloat16)


def draw_cache_keys(key, part):
    array_shape = (R, CACHE, KVH, HD)
    key_rows = jnp.clip(jax.random.normal(jax.random.fold_in(key, 103), array_shape, jnp.float32), -5.0, 5.0)
    return key_rows.astype(jnp.bfloat16)


def draw_retained_keys(key, part):
    array_shape = (R * GROUP, RET // GROUP, KVH, HD)
    key_rows = jnp.clip(jax.random.normal(jax.random.fold_in(key, 106), array_shape, jnp.float32) * 4.0, -24.0, 24.0)
    return key_rows.astype(jnp.bfloat16)


def draw_ancestors(key, part):
    random_bits = jax.random.randint(jax.random.fold_in(key, 107), (R, NODES), 0, 1 << 20)
    node_ids = jnp.arange(NODES, dtype=jnp.int32)
    parent_span = jnp.minimum(jnp.maximum(node_ids, 1), 8)
    parents = jnp.maximum(node_ids[None, :] - 1 - random_bits % parent_span[None, :], 0)
    identity = (node_ids[:, None] == node_ids[None, :]).astype(jnp.int32)
    ancestry = jnp.broadcast_to(identity, (R, NODES, NODES))
    request_ids = jnp.arange(R, dtype=jnp.int32)

    def extend(node_index, table):
        parent_row = table[request_ids, parents[:, node_index]]
        new_row = jnp.maximum(parent_row, (node_ids == node_index).astype(jnp.int32)[None, :])
        return table.at[:, node_index].set(new_row)
    return lax.fori_loop(1, NODES, extend, ancestry)


def set_ends(result, rng, least, largest):
    place = [jax.random.randint(jax.random.fold_in(rng, axis), (), 0, length) for axis, length in enumerate(result.shape)]
    widest = result.shape.index(max(result.shape))
    neighbour = place[:widest] + [(place[widest] + 1) % result.shape[widest]] + place[widest + 1:]
    return result.at[tuple(place)].set(least).at[tuple(neighbour)].set(largest)


def levels(rng, extent, pieces, low, top_value):
    gain = 1.0
    for dim, blocks in pieces:
        heights = jax.random.uniform(jax.random.fold_in(jax.random.fold_in(rng, 6), dim), (blocks,), jnp.float32, low / len(pieces), top_value / len(pieces))
        gain = gain * jnp.repeat(jnp.exp(heights), extent[dim] // blocks).reshape((-1,) + (1,) * (len(extent) - 1 - dim))
    return gain


def normal_values(rng, shape, width, reach, split=(), kind=jnp.bfloat16):
    loudness = levels(rng, shape, split, -0.22, 0.18) if split else 1.0
    values = jax.random.normal(rng, shape, jnp.float32) * width * loudness
    return jnp.minimum(jnp.maximum(values, -reach), reach).astype(kind)


def setup_inputs(seed: int = 0) -> dict:
    key_list = jax.random.split(jax.random.key(seed), 17)
    return {
        "tree_hidden": normal_values(key_list[0], (M, D), 1.0, 6.0, ((1, 8),)),
        "query_low": draw_query_low(jax.random.fold_in(key_list[16], 71), 0),
        "key_tree_low": normal_values(key_list[2], (M, KVH * HD), 3.5, 20.0, ((0, 8), (1, 4))),
        "value_tree_low": normal_values(key_list[3], (M, KVH * HD), 1.0, 6.0, ((0, 8), (1, 4))),
        "cache_keys": draw_cache_keys(jax.random.fold_in(key_list[16], 71), 0),
        "cache_values": normal_values(key_list[5], (R, CACHE, KVH, HD), 1.0, 6.0, ((1, 8), (2, 4))),
        "cache_lengths": jax.random.randint(key_list[6], (R,), CACHE // 8, CACHE + 1).astype(jnp.int32),
        "ancestors": draw_ancestors(jax.random.fold_in(key_list[16], 71), 0),
        "out_weight": normal_values(key_list[8], (HQ * HD, D), (HQ * HD) ** -0.5, 0.0625, ((0, 4), (1, 8))),
        "norm_gain": jnp.clip(1.0 + 0.18 * jax.random.normal(key_list[9], (D,), jnp.float32), 0.1, 1.9),
        "w_query_up": normal_values(key_list[10], (D, HQ * HD), D ** -0.5, 0.0625, ((0, 8), (1, 4))),
        "w_key_up": normal_values(key_list[11], (D, KVH * HD), (D // 64) ** -0.5, 0.5, ((0, 8), (1, 4))),
        "w_value_up": normal_values(key_list[12], (D, KVH * HD), D ** -0.5, 0.0625, ((0, 8), (1, 4))),
        "retained_keys": draw_retained_keys(jax.random.fold_in(key_list[16], 71), 0),
        "retained_values": normal_values(key_list[14], (R * GROUP, RET_PART, KVH, HD), 1.0, 6.0, ((0, 8), (2, 4))),
        "retained_index": set_ends(jax.random.randint(key_list[15], (R * GROUP, RET_PART, KVH), 0, CACHE), jax.random.fold_in(key_list[15], 1), 0, CACHE - 1).astype(jnp.int32),
    }


masked_score = -1e+30
norm_epsilon = 1e-05

def joint_attend(query_rows, far_keys, far_values, far_allowed, near_keys, near_values, near_mask):
    row_count = query_rows.shape[0]
    group_size = HQ // KVH
    queries = query_rows.astype(jnp.float32).reshape(row_count, KVH, group_size, HD).transpose(1, 0, 2, 3)
    near_key_rows = near_keys.astype(jnp.float32).reshape(-1, KVH, HD).transpose(1, 0, 2)
    near_value_rows = near_values.astype(jnp.float32).reshape(-1, KVH, HD).transpose(1, 0, 2)
    near_usable = near_mask > 0

    def one_head(operands):
        head_query, key_rows, value_rows, usable, tree_keys, tree_values = operands
        far_scores = jnp.einsum('ngd,cd->ngc', head_query, key_rows.astype(jnp.float32)) * HD ** (-0.5)
        near_scores = jnp.einsum('ngd,md->ngm', head_query, tree_keys) * HD ** (-0.5)
        scores = jnp.concatenate([far_scores, near_scores], axis=-1)
        allowed = jnp.concatenate([jnp.broadcast_to(usable[None, None, :], far_scores.shape), jnp.broadcast_to(near_usable[:, None, :], near_scores.shape)], axis=-1)
        masked = jnp.where(allowed, scores, masked_score)
        highest = lax.optimization_barrier(jnp.max(masked, axis=-1, keepdims=True))
        weights = jnp.where(allowed, jnp.exp(masked - highest), 0.0)
        weight_sum = lax.optimization_barrier(jnp.sum(weights, axis=-1, keepdims=True))
        rounded = lax.optimization_barrier(weights.astype(jnp.bfloat16)).astype(jnp.float32)
        both_values = jnp.concatenate([value_rows.astype(jnp.float32), tree_values], axis=0)
        return jnp.einsum('ngc,cd->ngd', rounded, both_values) / weight_sum
    blended = lax.map(one_head, (queries, far_keys.transpose(1, 0, 2), far_values.transpose(1, 0, 2), far_allowed.T, near_key_rows, near_value_rows))
    return blended.transpose(1, 0, 2, 3).reshape(row_count, HQ * HD).astype(jnp.float32)

def reference(tree_hidden, query_low, key_tree_low, value_tree_low, cache_keys, cache_values, cache_lengths, ancestors, out_weight, norm_gain, w_query_up, w_key_up, w_value_up, retained_keys, retained_values, retained_index):
    positions = jnp.arange(CACHE, dtype=jnp.int32)

    def lower_request(operands):
        query_rows, key_rows, value_rows, seq_length, tree_keys, tree_values, tree_mask = operands
        usable = jnp.broadcast_to((positions < seq_length)[:, None], (CACHE, KVH))
        return joint_attend(query_rows, key_rows, value_rows, usable, tree_keys, tree_values, tree_mask).astype(jnp.bfloat16)
    lower = lax.map(lower_request, (query_low.reshape(R, NODES, HQ * HD), cache_keys, cache_values, cache_lengths, key_tree_low.reshape(R, NODES, KVH * HD), value_tree_low.reshape(R, NODES, KVH * HD), ancestors)).reshape(R * NODES, HQ * HD)
    summed = jnp.dot(lower, out_weight, preferred_element_type=jnp.float32)
    residual = tree_hidden.astype(jnp.float32) + summed
    inverse = lax.rsqrt(lax.optimization_barrier(jnp.mean(residual * residual, axis=1, keepdims=True)) + norm_epsilon)
    normed = (residual * inverse * norm_gain[None, :]).astype(jnp.bfloat16)
    query_up = jnp.dot(normed, w_query_up, preferred_element_type=jnp.float32).astype(jnp.bfloat16)
    key_up = jnp.dot(normed, w_key_up, preferred_element_type=jnp.float32).astype(jnp.bfloat16)
    value_up = jnp.dot(normed, w_value_up, preferred_element_type=jnp.float32).astype(jnp.bfloat16)

    def upper_request(operands):
        query_rows, key_rows, value_rows, positions_kept, seq_length, tree_keys, tree_values, tree_mask = operands
        return joint_attend(query_rows, key_rows, value_rows, positions_kept < seq_length, tree_keys, tree_values, tree_mask)
    upper = lax.map(upper_request, (query_up.reshape(R, NODES, HQ * HD), retained_keys.reshape(R, RET, KVH, HD), retained_values.reshape(R, RET, KVH, HD), retained_index.reshape(R, RET, KVH), cache_lengths, key_up.reshape(R, NODES, KVH * HD), value_up.reshape(R, NODES, KVH * HD), ancestors)).reshape(R * NODES, HQ * HD)
    return (residual, upper)
```

```python
import functools

import jax
import jax.numpy as jnp
from jax import lax
from jax.experimental import pallas as pl
from jax.experimental.pallas import tpu as pltpu
from jax.sharding import PartitionSpec as P

MESH = pl.DeviceIdType.MESH
F32 = jnp.float32
BF16 = jnp.bfloat16
masked_score = -1e30
lowest_high = -1e29
norm_epsilon = 1e-05


def attend(queries, keys, values, allowed, scale):
    scores = lax.dot_general(
        queries, keys, (((1,), (1,)), ((), ())), preferred_element_type=F32
    ) * scale
    scores = jnp.where(allowed, scores, masked_score)
    high = jnp.maximum(jnp.max(scores, axis=1, keepdims=True), lowest_high)
    weights = jnp.exp(scores - high)
    total = jnp.sum(weights, axis=1, keepdims=True)
    blend = jnp.dot(weights.astype(BF16), values, preferred_element_type=F32)
    return blend, high, total


def kernel(
    sizes,
    lens_ref,
    q_ref,
    k_ref,
    v_ref,
    hid_ref,
    anc_ref,
    gain_ref,
    ridx_ref,
    ck_hbm,
    cv_hbm,
    ow_hbm,
    wk_hbm,
    wv_hbm,
    wq_hbm,
    rk_hbm,
    rv_hbm,
    res_ref,
    up_ref,
    ck,
    cv,
    ow,
    wk,
    wv,
    wq,
    rk,
    rv,
    form,
    low,
    part,
    stat,
    gpart,
    gstat,
    heads,
    terms,
    proj,
    gproj,
    upper,
    upart,
    ustat,
    ugpart,
    ugstat,
    load_sem,
    send_sem,
    recv_sem,
):
    S, T, R, own, kv, g, hd = sizes
    G = S // R
    M = S * own
    rows = own * g
    nodes = G * own
    scale = hd ** (-0.5)
    width = S * hid_ref.shape[1]
    me = lax.axis_index("seq")
    tp = lax.axis_index("tp")
    request = me // G
    base = request * G
    place = me - base

    barrier = pltpu.get_barrier_semaphore()
    for d in range(1, S):
        pl.semaphore_signal(
            barrier, inc=1, device_id={"seq": lax.rem(me + d, S)}, device_id_type=MESH
        )
    for d in range(1, T):
        pl.semaphore_signal(
            barrier, inc=1, device_id={"tp": lax.rem(tp + d, T)}, device_id_type=MESH
        )

    loads = []
    for i, (src, dst) in enumerate(
        (
            (ck_hbm, ck),
            (cv_hbm, cv),
            (ow_hbm, ow),
            (wk_hbm, wk),
            (wv_hbm, wv),
            (wq_hbm, wq),
            (rk_hbm, rk),
            (rv_hbm, rv),
        )
    ):
        copy = pltpu.make_async_copy(src, dst, load_sem.at[i])
        copy.start()
        loads.append(copy)

    sent = []

    def send(phase, d, src, dst, target):
        copy = pltpu.make_async_remote_copy(
            src_ref=src,
            dst_ref=dst,
            send_sem=send_sem.at[phase, d],
            recv_sem=recv_sem.at[phase, d],
            device_id=target,
            device_id_type=MESH,
        )
        copy.start()
        sent.append(copy)

    def arrive(phase, d, src, dst, target):
        pltpu.make_async_remote_copy(
            src_ref=src,
            dst_ref=dst,
            send_sem=send_sem.at[phase, d],
            recv_sem=recv_sem.at[phase, d],
            device_id=target,
            device_id_type=MESH,
        ).wait_recv()

    def peer(d):
        return lax.rem(me + d, S)

    def mate(d):
        return lax.rem(place + d, G)

    def spread(count, first, value):
        return value

    def tree_rows(block, j):
        return block[pl.ds(j, nodes, stride=g), :].astype(BF16)

    mask_rows = []
    node_start = place * own
    for r in range(own):
        row = anc_ref[request, pl.ds(node_start + r, 1), :]
        mask_rows.append(jnp.broadcast_to(row, (g, nodes)))
    tree_mask = jnp.concatenate(mask_rows, axis=0) > 0

    lanes = lax.broadcasted_iota(jnp.int32, (nodes * g, hd), 1)

    def pack_stats(stats):
        packed = jnp.zeros((nodes * g, hd), F32)
        for k, (high, total) in enumerate(stats):
            packed = jnp.where(lanes == 2 * k, high, packed)
            packed = jnp.where(lanes == 2 * k + 1, total, packed)
        return packed

    def finish(stats_ref, parts_ref, count, own_queries, tree_block):
        stats = [stats_ref[s] for s in range(count)]
        top = functools.reduce(jnp.maximum, stats)
        factors = [jnp.exp(x - top) for x in stats]
        done = []
        for k in range(kv):
            blend, high, total = attend(
                own_queries[k],
                tree_rows(tree_block, k),
                tree_rows(tree_block, kv + k),
                tree_mask,
                scale,
            )
            part_top = top[:, 2 * k : 2 * k + 1]
            highest = jnp.maximum(part_top, high)
            late = jnp.exp(high - highest)
            early = jnp.exp(part_top - highest)
            acc = jnp.zeros((rows, hd), F32)
            mass = jnp.zeros((rows, 1), F32)
            for s in range(count):
                factor = factors[s][:, 2 * k : 2 * k + 1]
                acc = acc + parts_ref[s, k].astype(F32) * factor
                mass = mass + stats[s][:, 2 * k + 1 : 2 * k + 2] * factor
            done.append((acc * early + blend * late) / (mass * early + total * late))
        return done

    form[kv] = jnp.zeros((M * g, hd), F32)
    q_rows = q_ref[...].astype(F32)
    k_rows = k_ref[...].astype(F32)
    v_rows = v_ref[...].astype(F32)
    for k in range(kv):
        for j in range(g):
            h = k * g + j
            form[k, pl.ds(j, own, stride=g), :] = q_rows[:, h * hd : (h + 1) * hd]
        form[kv, pl.ds(k, own, stride=g), :] = k_rows[:, k * hd : (k + 1) * hd]
        form[kv, pl.ds(kv + k, own, stride=g), :] = v_rows[:, k * hd : (k + 1) * hd]
    for k in range(kv + 1):
        low[me, k] = form[k, :rows, :].astype(BF16)

    pl.semaphore_wait(barrier, S - 1 + T - 1)

    for d in range(1, S):
        send(0, d, low.at[me], low.at[me], {"seq": peer(d)})
    loads[0].wait()
    loads[1].wait()
    for d in range(1, S):
        source = peer(S - d)
        arrive(0, d, low.at[source], low.at[source], {"seq": source})

    columns = ck.shape[1]
    column = lax.broadcasted_iota(jnp.int32, (1, columns), 1)
    first = me * (columns // kv)

    def cache_request(r, carry):
        limit = (lens_ref[r] - first) * kv
        stats = []
        for k in range(kv):
            queries = low[pl.ds(r * G, G), k].reshape(nodes * g, hd)
            allowed = jnp.logical_and(
                jnp.bitwise_and(column, kv - 1) == k, column < limit
            )
            blend, high, total = attend(queries, ck[r], cv[r], allowed, scale)
            stats.append((high, total))
            for a in range(G):
                part[r * G + a, k] = blend[a * rows : (a + 1) * rows].astype(BF16)
        packed = pack_stats(stats)
        for a in range(G):
            stat[r * G + a] = packed[a * rows : (a + 1) * rows]
        return carry

    if R == 1:
        cache_request(0, 0)
    else:
        lax.fori_loop(0, R, cache_request, 0)
    for d in range(1, S):
        target = peer(d)
        send(1, d, part.at[target], gpart.at[me], {"seq": target})
        send(2, d, stat.at[target], gstat.at[me], {"seq": target})
    gpart[me] = part[me]
    gstat[me] = stat[me]
    form[kv, : nodes * g, :] = low[pl.ds(base, G), kv].reshape(nodes * g, hd).astype(F32)
    own_queries = [low[me, k] for k in range(kv)]
    for d in range(1, S):
        source = peer(S - d)
        arrive(1, d, part.at[source], gpart.at[source], {"seq": source})
        arrive(2, d, stat.at[source], gstat.at[source], {"seq": source})

    done = finish(gstat, gpart, S, own_queries, form.at[kv])
    for k in range(kv):
        heads[me, k] = done[k].astype(BF16)
    for d in range(1, S):
        send(3, d, heads.at[me], heads.at[me], {"seq": peer(d)})
    loads[2].wait()
    for d in range(1, S):
        source = peer(S - d)
        arrive(3, d, heads.at[source], heads.at[source], {"seq": source})

    for k in range(kv):
        form[k] = heads[:, k].reshape(M * g, hd).astype(F32)
    lower = jnp.concatenate(
        [
            form[k, pl.ds(j, M, stride=g), :].astype(BF16)
            for k in range(kv)
            for j in range(g)
        ],
        axis=1,
    )
    terms[tp] = jnp.dot(lower, ow[...], preferred_element_type=F32).astype(BF16)
    for d in range(1, T):
        send(4, d, terms.at[tp], terms.at[tp], {"tp": lax.rem(tp + d, T)})
    loads[3].wait()
    loads[4].wait()
    loads[5].wait()
    for d in range(1, T):
        source = lax.rem(tp + T - d, T)
        arrive(4, d, terms.at[source], terms.at[source], {"tp": source})
    residual = hid_ref[...].astype(F32)
    summed = terms[0].astype(F32)
    for t in range(1, T):
        summed = summed + terms[t].astype(F32)
    residual = residual + summed
    res_ref[...] = residual

    squares = jnp.broadcast_to(jnp.sum(residual * residual, axis=1, keepdims=True), (M, hd))
    coarse = squares.astype(BF16).astype(F32)
    scaled = (residual * gain_ref[...]).astype(BF16)
    query_terms = jnp.dot(scaled, wq[...], preferred_element_type=F32)
    key_terms = jnp.dot(scaled, wk[...], preferred_element_type=F32)
    value_terms = jnp.dot(scaled, wv[...], preferred_element_type=F32)
    form[kv] = jnp.zeros((M * g, hd), F32)
    for k in range(kv):
        for j in range(g):
            h = k * g + j
            form[k, pl.ds(j, M, stride=g), :] = query_terms[:, h * hd : (h + 1) * hd]
        form[kv, pl.ds(k, M, stride=g), :] = key_terms[:, k * hd : (k + 1) * hd]
        form[kv, pl.ds(kv + k, M, stride=g), :] = value_terms[:, k * hd : (k + 1) * hd]
    form[kv, pl.ds(2 * kv, M, stride=g), :] = coarse
    form[kv, pl.ds(2 * kv + 1, M, stride=g), :] = squares - coarse
    for s in range(S):
        for k in range(kv + 1):
            proj[s, k] = form[k, s * rows : (s + 1) * rows, :].astype(BF16)
    for d in range(1, S):
        target = peer(d)
        send(5, d, proj.at[target], gproj.at[me], {"seq": target})
    gproj[me] = proj[me]
    for d in range(1, S):
        source = peer(S - d)
        arrive(5, d, proj.at[source], gproj.at[source], {"seq": source})
    sums = []
    for k in range(kv + 1):
        total = gproj[0, k].astype(F32)
        for s in range(1, S):
            total = total + gproj[s, k].astype(F32)
        sums.append(total)
    inverses = []
    for r in range(own):
        at = r * g + 2 * kv
        square = sums[kv][at : at + 1, :] + sums[kv][at + 1 : at + 2, :]
        inverse = lax.rsqrt(square / width + norm_epsilon)
        inverses.append(jnp.broadcast_to(inverse, (g, hd)))
    inverse = jnp.concatenate(inverses, axis=0)

    own_queries = []
    for k in range(kv + 1):
        block = (sums[k] * inverse).astype(BF16)
        upper[place, k] = block
        own_queries.append(block)
    for d in range(1, G):
        send(6, d, upper.at[place], upper.at[place], {"seq": base + mate(d)})
    loads[6].wait()
    loads[7].wait()
    for d in range(1, G):
        source = mate(G - d)
        arrive(6, d, upper.at[source], upper.at[source], {"seq": base + source})

    entries = rk.shape[0]
    entry = lax.broadcasted_iota(jnp.int32, (1, entries), 1)
    kept = ridx_ref[...] < lens_ref[request]
    stats = []
    for k in range(kv):
        allowed = jnp.logical_and(jnp.bitwise_and(entry, kv - 1) == k, kept)
        queries = upper[:, k].reshape(nodes * g, hd)
        blend, high, total = attend(queries, rk[...], rv[...], allowed, scale)
        stats.append((high, total))
        for a in range(G):
            upart[a, k] = blend[a * rows : (a + 1) * rows].astype(BF16)
    packed = pack_stats(stats)
    for a in range(G):
        ustat[a] = packed[a * rows : (a + 1) * rows]
    for d in range(1, G):
        target = mate(d)
        send(7, d, upart.at[target], ugpart.at[place], {"seq": base + target})
        send(8, d, ustat.at[target], ugstat.at[place], {"seq": base + target})
    ugpart[place] = upart[place]
    ugstat[place] = ustat[place]
    form[kv, : nodes * g, :] = upper[:, kv].reshape(nodes * g, hd).astype(F32)
    for d in range(1, G):
        source = mate(G - d)
        arrive(7, d, upart.at[source], ugpart.at[source], {"seq": base + source})
        arrive(8, d, ustat.at[source], ugstat.at[source], {"seq": base + source})
    done = finish(ugstat, ugpart, G, own_queries, form.at[kv])
    for k in range(kv):
        form[k, :rows, :] = done[k]
        for j in range(g):
            h = k * g + j
            up_ref[:, h * hd : (h + 1) * hd] = form[k, pl.ds(j, own, stride=g), :]
    for copy in sent:
        copy.wait_send()


def shards(
    tree_hidden,
    query_low,
    key_tree_low,
    value_tree_low,
    cache_keys,
    cache_values,
    cache_lengths,
    ancestors,
    out_weight,
    norm_gain,
    w_query_up,
    w_key_up,
    w_value_up,
    retained_keys,
    retained_values,
    retained_index,
):
    S = lax.axis_size("seq")
    T = lax.axis_size("tp")
    R, part, kv, hd = cache_keys.shape
    own, row_width = query_low.shape
    g = row_width // (kv * hd)
    G = S // R
    M = S * own
    rows = own * g
    features = tree_hidden.shape[1]
    entries = retained_keys.shape[1] * kv
    ck = cache_keys.reshape(R, part * kv, hd)
    cv = cache_values.reshape(R, part * kv, hd)
    rk = retained_keys.reshape(entries, hd)
    rv = retained_values.reshape(entries, hd)
    ridx = retained_index.reshape(1, entries)
    gain = norm_gain.reshape(1, features)
    vmem = pl.BlockSpec(memory_space=pltpu.VMEM)
    hbm = pl.BlockSpec(memory_space=pl.ANY)
    big = (ck, cv, out_weight, w_key_up, w_value_up, w_query_up, rk, rv)
    return pl.pallas_call(
        functools.partial(kernel, (S, T, R, own, kv, g, hd)),
        out_shape=(
            jax.ShapeDtypeStruct((M, features), F32),
            jax.ShapeDtypeStruct((own, row_width), F32),
        ),
        in_specs=[pl.BlockSpec(memory_space=pltpu.SMEM)] + [vmem] * 7 + [hbm] * 8,
        out_specs=(vmem, vmem),
        scratch_shapes=[pltpu.VMEM(x.shape, x.dtype) for x in big]
        + [
            pltpu.VMEM((kv + 1, M * g, hd), F32),
            pltpu.VMEM((S, kv + 1, rows, hd), BF16),
            pltpu.VMEM((S, kv, rows, hd), BF16),
            pltpu.VMEM((S, rows, hd), F32),
            pltpu.VMEM((S, kv, rows, hd), BF16),
            pltpu.VMEM((S, rows, hd), F32),
            pltpu.VMEM((S, kv, rows, hd), BF16),
            pltpu.VMEM((T, M, features), BF16),
            pltpu.VMEM((S, kv + 1, rows, hd), BF16),
            pltpu.VMEM((S, kv + 1, rows, hd), BF16),
            pltpu.VMEM((G, kv + 1, rows, hd), BF16),
            pltpu.VMEM((G, kv, rows, hd), BF16),
            pltpu.VMEM((G, rows, hd), F32),
            pltpu.VMEM((G, kv, rows, hd), BF16),
            pltpu.VMEM((G, rows, hd), F32),
            pltpu.SemaphoreType.DMA((len(big),)),
            pltpu.SemaphoreType.DMA((9, max(S, T))),
            pltpu.SemaphoreType.DMA((9, max(S, T))),
        ],
        compiler_params=pltpu.CompilerParams(
            collective_id=0, has_side_effects=True, vmem_limit_bytes=56 * 1024 * 1024
        ),
        name="two_layers",
    )(
        cache_lengths,
        query_low,
        key_tree_low,
        value_tree_low,
        tree_hidden,
        ancestors,
        gain,
        ridx,
        *big,
    )


def solution(mesh):
    return jax.shard_map(
        shards,
        mesh=mesh,
        in_specs=(
            P(None, "seq"),
            P("seq", "tp"),
            P("seq", "tp"),
            P("seq", "tp"),
            P(None, "seq", "tp", None),
            P(None, "seq", "tp", None),
            P(),
            P(),
            P("tp", "seq"),
            P("seq"),
            P("seq", "tp"),
            P("seq", "tp"),
            P("seq", "tp"),
            P("seq", None, "tp", None),
            P("seq", None, "tp", None),
            P("seq", None, "tp"),
        ),
        out_specs=(P(None, "seq"), P("seq", "tp")),
        check_vma=False,
    )
```

```python
import functools

import jax
import jax.numpy as jnp
from jax import lax
from jax.experimental import pallas as pl
from jax.experimental.pallas import tpu as pltpu
from jax.sharding import PartitionSpec as P

MESH = pl.DeviceIdType.MESH
F32 = jnp.float32
BF16 = jnp.bfloat16
masked_score = -1e30
lowest_high = -1e29
norm_epsilon = 1e-05


def attend(queries, keys, values, allowed, scale):
    scores = lax.dot_general(
        queries, keys, (((1,), (1,)), ((), ())), preferred_element_type=F32
    ) * scale
    scores = jnp.where(allowed, scores, masked_score)
    high = jnp.maximum(jnp.max(scores, axis=1, keepdims=True), lowest_high)
    weights = jnp.exp(scores - high)
    total = jnp.sum(weights, axis=1, keepdims=True)
    blend = jnp.dot(weights.astype(BF16), values, preferred_element_type=F32)
    return blend, high, total


def kernel(
    sizes,
    lens_hbm,
    q_hbm,
    k_hbm,
    v_hbm,
    ck_hbm,
    cv_hbm,
    anc_hbm,
    ow_hbm,
    hid_hbm,
    gain_hbm,
    wk_hbm,
    wv_hbm,
    wq_hbm,
    ridx_hbm,
    rk_hbm,
    rv_hbm,
    res_ref,
    up_ref,
    lens_ref,
    q_ref,
    k_ref,
    v_ref,
    ck,
    cv,
    anc_ref,
    ow,
    hid_ref,
    gain_ref,
    wk,
    wv,
    wq,
    ridx_ref,
    rk,
    rv,
    form,
    low,
    part,
    gpart,
    heads,
    terms,
    proj,
    gproj,
    upper,
    upart,
    ugpart,
    load_sem,
    send_sem,
    recv_sem,
):
    S, T, R, own, kv, g, hd = sizes
    G = S // R
    M = S * own
    rows = own * g
    nodes = G * own
    scale = hd ** (-0.5)
    width = S * hid_ref.shape[1]
    me = lax.axis_index("seq")
    tp = lax.axis_index("tp")
    request = me // G
    base = request * G
    place = me - base

    barrier = pltpu.get_barrier_semaphore()
    for d in range(1, S):
        pl.semaphore_signal(
            barrier, inc=1, device_id={"seq": lax.rem(me + d, S)}, device_id_type=MESH
        )
    for d in range(1, T):
        pl.semaphore_signal(
            barrier, inc=1, device_id={"tp": lax.rem(tp + d, T)}, device_id_type=MESH
        )

    loads = []
    for i, (src, dst) in enumerate(
        (
            (q_hbm, q_ref),
            (k_hbm, k_ref),
            (v_hbm, v_ref),
            (ck_hbm, ck),
            (cv_hbm, cv),
            (anc_hbm, anc_ref),
            (ow_hbm, ow),
            (hid_hbm, hid_ref),
            (gain_hbm, gain_ref),
            (wk_hbm, wk),
            (wv_hbm, wv),
            (wq_hbm, wq),
            (ridx_hbm, ridx_ref),
            (rk_hbm, rk),
            (rv_hbm, rv),
            (lens_hbm, lens_ref),
        )
    ):
        copy = pltpu.make_async_copy(src, dst, load_sem.at[i])
        copy.start()
        loads.append(copy)

    sent = []

    def send(phase, d, src, dst, target):
        copy = pltpu.make_async_remote_copy(
            src_ref=src,
            dst_ref=dst,
            send_sem=send_sem.at[phase, d],
            recv_sem=recv_sem.at[phase, d],
            device_id=target,
            device_id_type=MESH,
        )
        copy.start()
        sent.append(copy)

    def arrive(phase, d, src, dst, target):
        pltpu.make_async_remote_copy(
            src_ref=src,
            dst_ref=dst,
            send_sem=send_sem.at[phase, d],
            recv_sem=recv_sem.at[phase, d],
            device_id=target,
            device_id_type=MESH,
        ).wait_recv()

    def peer(d):
        return lax.rem(me + d, S)

    def mate(d):
        return lax.rem(place + d, G)

    def tree_rows(block, j):
        return block[pl.ds(j, nodes, stride=g), :].astype(BF16)

    lanes = lax.broadcasted_iota(jnp.int32, (nodes * g, hd), 1)

    third = 32

    def pack_stats(stats):
        packed = jnp.zeros((nodes * g, hd), F32)
        spot = jnp.bitwise_and(lanes, third - 1)
        for k, (high, total) in enumerate(stats):
            packed = jnp.where(spot == 2 * k, high, packed)
            packed = jnp.where(spot == 2 * k + 1, total, packed)
        coarse = packed.astype(BF16).astype(F32)
        rest = packed - coarse
        middle = rest.astype(BF16).astype(F32)
        fine = rest - middle
        packed = jnp.where(lanes < third, coarse, jnp.where(lanes < 2 * third, middle, fine))
        return jnp.where(lanes < 3 * third, packed, 0.0).astype(BF16)

    def unpack_stats(block):
        packed = block.astype(F32)
        return (packed + pltpu.roll(packed, hd - third, 1)) + pltpu.roll(packed, hd - 2 * third, 1)

    def tree_part(own_queries, tree_block, tree_mask):
        return [
            attend(
                own_queries[k],
                tree_rows(tree_block, k),
                tree_rows(tree_block, kv + k),
                tree_mask,
                scale,
            )
            for k in range(kv)
        ]

    def finish(parts_ref, count, trees):
        stats = [unpack_stats(parts_ref[s, kv]) for s in range(count)]
        top = functools.reduce(jnp.maximum, stats)
        factors = [jnp.exp(x - top) for x in stats]
        done = []
        for k in range(kv):
            blend, high, total = trees[k]
            part_top = top[:, 2 * k : 2 * k + 1]
            highest = jnp.maximum(part_top, high)
            late = jnp.exp(high - highest)
            early = jnp.exp(part_top - highest)
            acc = jnp.zeros((rows, hd), F32)
            mass = jnp.zeros((rows, 1), F32)
            for s in range(count):
                factor = factors[s][:, 2 * k : 2 * k + 1]
                acc = acc + parts_ref[s, k].astype(F32) * factor
                mass = mass + stats[s][:, 2 * k + 1 : 2 * k + 2] * factor
            done.append((acc * early + blend * late) / (mass * early + total * late))
        return done

    form[kv] = jnp.zeros((M * g, hd), F32)
    for i in range(3):
        loads[i].wait()
    q_rows = q_ref[...].astype(F32)
    k_rows = k_ref[...].astype(F32)
    v_rows = v_ref[...].astype(F32)
    for k in range(kv):
        for j in range(g):
            h = k * g + j
            form[k, pl.ds(j, own, stride=g), :] = q_rows[:, h * hd : (h + 1) * hd]
        form[kv, pl.ds(k, own, stride=g), :] = k_rows[:, k * hd : (k + 1) * hd]
        form[kv, pl.ds(kv + k, own, stride=g), :] = v_rows[:, k * hd : (k + 1) * hd]
    for k in range(kv + 1):
        low[me, k] = form[k, :rows, :].astype(BF16)

    pl.semaphore_wait(barrier, S - 1 + T - 1)

    for d in range(1, S):
        own_q = low.at[me, pl.ds(0, kv)]
        send(0, d, own_q, own_q, {"seq": peer(d)})
    for d in range(1, S):
        own_kv = low.at[me, pl.ds(kv, 1)]
        send(2, d, own_kv, own_kv, {"seq": peer(d)})
    loads[3].wait()
    loads[4].wait()
    loads[5].wait()
    loads[15].wait()
    mask_rows = []
    node_start = place * own
    for r in range(own):
        row = anc_ref[request, pl.ds(node_start + r, 1), :]
        mask_rows.append(jnp.broadcast_to(row, (g, nodes)))
    tree_mask = jnp.concatenate(mask_rows, axis=0) > 0
    for d in range(1, S):
        source = peer(S - d)
        there = low.at[source, pl.ds(0, kv)]
        arrive(0, d, there, there, {"seq": source})

    columns = ck.shape[1]
    column = lax.broadcasted_iota(jnp.int32, (1, columns), 1)
    first = me * (columns // kv)

    def cache_request(r, carry):
        limit = (lens_ref[r] - first) * kv
        stats = []
        for k in range(kv):
            queries = low[pl.ds(r * G, G), k].reshape(nodes * g, hd)
            allowed = jnp.logical_and(
                jnp.bitwise_and(column, kv - 1) == k, column < limit
            )
            blend, high, total = attend(queries, ck[r], cv[r], allowed, scale)
            stats.append((high, total))
            for a in range(G):
                part[r * G + a, k] = blend[a * rows : (a + 1) * rows].astype(BF16)
        packed = pack_stats(stats)
        for a in range(G):
            part[r * G + a, kv] = packed[a * rows : (a + 1) * rows]
        return carry

    if R == 1:
        cache_request(0, 0)
    else:
        lax.fori_loop(0, R, cache_request, 0)
    for d in range(1, S):
        target = peer(d)
        send(1, d, part.at[target], gpart.at[me], {"seq": target})
    gpart[me] = part[me]
    for d in range(1, S):
        source = peer(S - d)
        there = low.at[source, pl.ds(kv, 1)]
        arrive(2, d, there, there, {"seq": source})
    form[kv, : nodes * g, :] = low[pl.ds(base, G), kv].reshape(nodes * g, hd).astype(F32)
    trees = tree_part([low[me, k] for k in range(kv)], form.at[kv], tree_mask)
    for d in range(1, S):
        source = peer(S - d)
        arrive(1, d, part.at[source], gpart.at[source], {"seq": source})

    done = finish(gpart, S, trees)
    for k in range(kv):
        heads[me, k] = done[k].astype(BF16)
    for d in range(1, S):
        send(3, d, heads.at[me], heads.at[me], {"seq": peer(d)})
    loads[6].wait()
    for d in range(1, S):
        source = peer(S - d)
        arrive(3, d, heads.at[source], heads.at[source], {"seq": source})

    for k in range(kv):
        form[k] = heads[:, k].reshape(M * g, hd).astype(F32)
    lower = jnp.concatenate(
        [
            form[k, pl.ds(j, M, stride=g), :].astype(BF16)
            for k in range(kv)
            for j in range(g)
        ],
        axis=1,
    )
    terms[tp] = jnp.dot(lower, ow[...], preferred_element_type=F32).astype(BF16)
    for d in range(1, T):
        send(4, d, terms.at[tp], terms.at[tp], {"tp": lax.rem(tp + d, T)})
    for i in range(7, 12):
        loads[i].wait()
    for d in range(1, T):
        source = lax.rem(tp + T - d, T)
        arrive(4, d, terms.at[source], terms.at[source], {"tp": source})
    residual = hid_ref[...].astype(F32)
    summed = terms[0].astype(F32)
    for t in range(1, T):
        summed = summed + terms[t].astype(F32)
    residual = residual + summed
    res_ref[...] = residual

    squares = jnp.broadcast_to(jnp.sum(residual * residual, axis=1, keepdims=True), (M, hd))
    coarse = squares.astype(BF16).astype(F32)
    scaled = (residual * gain_ref[...]).astype(BF16)
    query_terms = jnp.dot(scaled, wq[...], preferred_element_type=F32)
    key_terms = jnp.dot(scaled, wk[...], preferred_element_type=F32)
    value_terms = jnp.dot(scaled, wv[...], preferred_element_type=F32)
    form[kv] = jnp.zeros((M * g, hd), F32)
    for k in range(kv):
        for j in range(g):
            h = k * g + j
            form[k, pl.ds(j, M, stride=g), :] = query_terms[:, h * hd : (h + 1) * hd]
        form[kv, pl.ds(k, M, stride=g), :] = key_terms[:, k * hd : (k + 1) * hd]
        form[kv, pl.ds(kv + k, M, stride=g), :] = value_terms[:, k * hd : (k + 1) * hd]
    form[kv, pl.ds(2 * kv, M, stride=g), :] = coarse
    form[kv, pl.ds(2 * kv + 1, M, stride=g), :] = squares - coarse
    for s in range(S):
        for k in range(kv + 1):
            proj[s, k] = form[k, s * rows : (s + 1) * rows, :].astype(BF16)
    for d in range(1, S):
        target = peer(d)
        send(5, d, proj.at[target], gproj.at[me], {"seq": target})
    gproj[me] = proj[me]
    for d in range(1, S):
        source = peer(S - d)
        arrive(5, d, proj.at[source], gproj.at[source], {"seq": source})
    sums = []
    for k in range(kv + 1):
        total = gproj[0, k].astype(F32)
        for s in range(1, S):
            total = total + gproj[s, k].astype(F32)
        sums.append(total)
    inverses = []
    for r in range(own):
        at = r * g + 2 * kv
        square = sums[kv][at : at + 1, :] + sums[kv][at + 1 : at + 2, :]
        inverse = lax.rsqrt(square / width + norm_epsilon)
        inverses.append(jnp.broadcast_to(inverse, (g, hd)))
    inverse = jnp.concatenate(inverses, axis=0)

    own_queries = []
    for k in range(kv + 1):
        block = (sums[k] * inverse).astype(BF16)
        upper[place, k] = block
        own_queries.append(block)
    for d in range(1, G):
        own_q = upper.at[place, pl.ds(0, kv)]
        send(6, d, own_q, own_q, {"seq": base + mate(d)})
    for d in range(1, G):
        own_kv = upper.at[place, pl.ds(kv, 1)]
        send(8, d, own_kv, own_kv, {"seq": base + mate(d)})
    for i in range(12, 15):
        loads[i].wait()
    entries = rk.shape[0]
    chunk = min(hd, entries // kv)
    at_row = lax.broadcasted_iota(jnp.int32, (chunk, chunk * kv), 0)
    at_column = lax.broadcasted_iota(jnp.int32, (chunk, chunk * kv), 1)
    length_here = lens_ref[request]
    kept = []
    for k in range(kv):
        place_of = jnp.where(at_column == at_row * kv + k, 1.0, 0.0).astype(BF16)
        pieces = []
        for c in range(entries // kv // chunk):
            index_row = ridx_ref[k : k + 1, c * chunk : (c + 1) * chunk]
            flag = jnp.where(index_row < length_here, 1.0, 0.0)
            flag = jnp.broadcast_to(flag, (16, chunk)).astype(BF16)
            pieces.append(jnp.dot(flag, place_of, preferred_element_type=F32)[0:1, :])
        kept.append(jnp.concatenate(pieces, axis=1))
    for d in range(1, G):
        source = mate(G - d)
        there = upper.at[source, pl.ds(0, kv)]
        arrive(6, d, there, there, {"seq": base + source})

    stats = []
    for k in range(kv):
        allowed = kept[k] > 0.5
        queries = upper[:, k].reshape(nodes * g, hd)
        blend, high, total = attend(queries, rk[...], rv[...], allowed, scale)
        stats.append((high, total))
        for a in range(G):
            upart[a, k] = blend[a * rows : (a + 1) * rows].astype(BF16)
    packed = pack_stats(stats)
    for a in range(G):
        upart[a, kv] = packed[a * rows : (a + 1) * rows]
    for d in range(1, G):
        target = mate(d)
        send(7, d, upart.at[target], ugpart.at[place], {"seq": base + target})
    ugpart[place] = upart[place]
    for d in range(1, G):
        source = mate(G - d)
        there = upper.at[source, pl.ds(kv, 1)]
        arrive(8, d, there, there, {"seq": base + source})
    form[kv, : nodes * g, :] = upper[:, kv].reshape(nodes * g, hd).astype(F32)
    trees = tree_part(own_queries, form.at[kv], tree_mask)
    for d in range(1, G):
        source = mate(G - d)
        arrive(7, d, upart.at[source], ugpart.at[source], {"seq": base + source})
    done = finish(ugpart, G, trees)
    for k in range(kv):
        form[k, :rows, :] = done[k]
        for j in range(g):
            h = k * g + j
            up_ref[:, h * hd : (h + 1) * hd] = form[k, pl.ds(j, own, stride=g), :]
    for copy in sent:
        copy.wait_send()


def shards(
    tree_hidden,
    query_low,
    key_tree_low,
    value_tree_low,
    cache_keys,
    cache_values,
    cache_lengths,
    ancestors,
    out_weight,
    norm_gain,
    w_query_up,
    w_key_up,
    w_value_up,
    retained_keys,
    retained_values,
    retained_index,
):
    S = lax.axis_size("seq")
    T = lax.axis_size("tp")
    R, part, kv, hd = cache_keys.shape
    own, row_width = query_low.shape
    g = row_width // (kv * hd)
    G = S // R
    M = S * own
    rows = own * g
    features = tree_hidden.shape[1]
    entries = retained_keys.shape[1] * kv
    ck = cache_keys.reshape(R, part * kv, hd)
    cv = cache_values.reshape(R, part * kv, hd)
    rk = retained_keys.reshape(entries, hd)
    rv = retained_values.reshape(entries, hd)
    ridx = retained_index[0].T
    gain = norm_gain.reshape(1, features)
    vmem = pl.BlockSpec(memory_space=pltpu.VMEM)
    hbm = pl.BlockSpec(memory_space=pl.ANY)
    big = (
        query_low,
        key_tree_low,
        value_tree_low,
        ck,
        cv,
        ancestors,
        out_weight,
        tree_hidden,
        gain,
        w_key_up,
        w_value_up,
        w_query_up,
        ridx,
        rk,
        rv,
    )
    outs = pl.pallas_call(
        functools.partial(kernel, (S, T, R, own, kv, g, hd)),
        out_shape=(
            jax.ShapeDtypeStruct((M, features), F32),
            jax.ShapeDtypeStruct((own, row_width), F32),
        ),
        in_specs=[pl.BlockSpec(memory_space=pltpu.HBM)] + [hbm] * len(big),
        out_specs=(vmem, vmem),
        scratch_shapes=[pltpu.SMEM((R,), jnp.int32)]
        + [pltpu.VMEM(x.shape, x.dtype) for x in big]
        + [
            pltpu.VMEM((kv + 1, M * g, hd), F32),
            pltpu.VMEM((S, kv + 1, rows, hd), BF16),
            pltpu.VMEM((S, kv + 1, rows, hd), BF16),
            pltpu.VMEM((S, kv + 1, rows, hd), BF16),
            pltpu.VMEM((S, kv, rows, hd), BF16),
            pltpu.VMEM((T, M, features), BF16),
            pltpu.VMEM((S, kv + 1, rows, hd), BF16),
            pltpu.VMEM((S, kv + 1, rows, hd), BF16),
            pltpu.VMEM((G, kv + 1, rows, hd), BF16),
            pltpu.VMEM((G, kv + 1, rows, hd), BF16),
            pltpu.VMEM((G, kv + 1, rows, hd), BF16),
            pltpu.SemaphoreType.DMA((1 + len(big),)),
            pltpu.SemaphoreType.DMA((9, max(S, T))),
            pltpu.SemaphoreType.DMA((9, max(S, T))),
        ],
        compiler_params=pltpu.CompilerParams(
            collective_id=0, has_side_effects=True, vmem_limit_bytes=56 * 1024 * 1024
        ),
        name="two_layers",
    )(
        cache_lengths,
        *big,
    )

    def settle(a_ref, b_ref, c_ref, d_ref):
        c_ref[...] = a_ref[...]
        d_ref[...] = b_ref[...]

    return pl.pallas_call(
        settle,
        out_shape=tuple(jax.ShapeDtypeStruct(x.shape, x.dtype) for x in outs),
        in_specs=[vmem] * 2,
        out_specs=(vmem, vmem),
        name="settle",
    )(*outs)


def solution(mesh):
    return jax.shard_map(
        shards,
        mesh=mesh,
        in_specs=(
            P(None, "seq"),
            P("seq", "tp"),
            P("seq", "tp"),
            P("seq", "tp"),
            P(None, "seq", "tp", None),
            P(None, "seq", "tp", None),
            P(),
            P(),
            P("tp", "seq"),
            P("seq"),
            P("seq", "tp"),
            P("seq", "tp"),
            P("seq", "tp"),
            P("seq", None, "tp", None),
            P("seq", None, "tp", None),
            P("seq", None, "tp"),
        ),
        out_specs=(P(None, "seq"), P("seq", "tp")),
        check_vma=False,
    )
```
